32 devices in a mesh: dp: 2 (over y), ep: 16 (over z, x, core).
Axes of the slice: x: 2, y: 2, z: 4, core: 2. Of those that a mesh axis runs over, the one named last changes fastest.
Arguments:
- tokens: bfloat16 [16, 2, 1, 3584], P('ep', 'dp'), may hold values from -6 to 6
- gate_weights: bfloat16 [16, 2, 1, 8], P('ep', 'dp'), may hold values from 0.099609375 to 0.59765625
- expert_ids: int32 [16, 2, 1, 8], P('ep', 'dp'), may hold values from 0 to 15, all different within a row; in each aligned block of 2 rows (0 to 1, 2 to 3, ..., all dimensions but the last counted through in order) at most 2 rows name the same one
- gate_proj: bfloat16 [16, 3584, 2048], P('ep', None, 'dp'), may hold values from -0.09375 to 0.09375
- up_proj: bfloat16 [16, 3584, 2048], P('ep', None, 'dp'), may hold values from -0.09375 to 0.09375
- down_proj: bfloat16 [16, 2048, 3584], P('ep', 'dp'), may hold values from -0.125 to 0.125
Outputs:
- mixed: bfloat16 [16, 2, 1, 3584], P('ep', 'dp')
The draws below stay inside these ranges and needn't reach their ends.
Inputs may be any that keep to these rules, and one draw needn't show every extreme that they name: `expert_ids`: each token names 8 different experts. Among the 2 tokens of one index of the first dimension, no expert is named more than 2 times, a bound that some block reaches.
All inputs are finite; a program needn't handle non-finite values.
Results may differ from the reference program's by a relative error of at most 0.02.
Values may be sent and summed in bfloat16 or wider, within the bound.
No kernel may reach another device: no remote copies, remote signals or barrier semaphores. Data moves between devices by JAX's collectives and lax.ppermute only.
A program may use at most 64 MiB of HBM per device.

```python
import math
import jax
import jax.numpy as jnp
import numpy as np
from jax import lax

D = 3584
FF = 2048
TOP = 8
TOK_DEV = 1
CAP = 2
EXPERTS = 16
N_DP = 2
N_EP = 16


def level_of(rng, shape, pieces, smallest, largest):
    factor_of = 1.0
    for dim, shards_of in pieces:
        steps = jax.random.uniform(jax.random.fold_in(jax.random.fold_in(rng, 6), dim), (shards_of,), jnp.float32, smallest / len(pieces), largest / len(pieces))
        factor_of = factor_of * jnp.repeat(jnp.exp(steps), shape[dim] // shards_of).reshape((-1,) + (1,) * (len(shape) - 1 - dim))
    return factor_of


def routed_block(own_key, own, number, rows, amount, top, most, lean):
    sequence = jax.random.permutation(own_key, amount)
    crowded, usual = portions_of(amount, rows * top, most, lean, True), portions_of(amount, rows * top, most, lean, False)
    places = jnp.arange(amount)

    def named(lengths, rotation):
        used = int((lengths > 0).sum())
        fixed = max(1, used // 4)
        passed = fixed + (places - fixed + rotation * (used - fixed)) % max(1, amount - fixed)
        return jnp.zeros((amount,), jnp.int32).at[sequence[jnp.where(places < fixed, places, passed)]].set(jnp.asarray(lengths, jnp.int32))

    lengths = jnp.where(number % 4 == 0, named(crowded, number // 4), named(usual, number - number // 4 - 1))
    mixed = jax.random.permutation(jax.random.fold_in(own, 3), amount)
    giver, receiver = mixed[0:amount // 2 * 2:2], mixed[1:amount // 2 * 2:2]
    margin = jnp.minimum(lengths[giver] - 1, most - lengths[receiver]) // 2
    margin = jnp.where((giver == sequence[0]) | (receiver == sequence[0]) | (lengths[receiver] == 0), 0, jnp.maximum(margin, 0))
    passed = jax.random.randint(jax.random.fold_in(own, 4), (amount // 2,), 0, 1 << 20) % (margin + 1)
    lengths = lengths.at[giver].add(-passed).at[receiver].add(passed)
    items = jnp.searchsorted(jnp.cumsum(lengths), jnp.arange(rows * top), side="right").astype(jnp.int32)
    listing = items.reshape(top, rows).T
    listing = listing[jax.random.permutation(jax.random.fold_in(own, 1), rows)]
    rotation = jax.random.randint(jax.random.fold_in(own, 2), (rows, 1), 0, top)
    return jnp.take_along_axis(listing, (jnp.arange(top)[None, :] + rotation) % top, axis=1)


def portions_of(number_of, total, reach, slope, full):
    loads = [(1 << 20) // math.isqrt(grade ** slope) + 1 for grade in range(1, number_of + 1)]
    largest = reach if full else min(reach, max(-(-total // number_of), total * loads[0] // sum(loads)))
    least = 1 if total - largest >= number_of - 1 else 0
    counts, rest = [largest] + [least] * (number_of - 1), total - largest - least * (number_of - 1)
    while rest > 0:
        candidates = [i for i in range(1, number_of) if counts[i] < largest] or [i for i in range(1, number_of) if counts[i] < reach]
        whole, budget = sum([loads[i] for i in candidates]), rest
        for i in candidates:
            addition = min(reach - counts[i], max(1, budget * loads[i] // whole), rest)
            counts[i] = counts[i] + addition
            rest = rest - addition
    return np.array(counts)


def scatter_about(key, dims, spread, limit, split=(), kind=jnp.bfloat16):
    factor_of = level_of(key, dims, split, -0.22, 0.18) if split else 1.0
    entries = jax.random.normal(key, dims, jnp.float32) * spread * factor_of
    return jnp.minimum(jnp.maximum(entries, -limit), limit).astype(kind)


def setup_inputs(seed: int = 0) -> dict:
    streams_of = jax.random.split(jax.random.key(seed), 7)
    tokens = scatter_about(streams_of[0], (N_EP, N_DP, TOK_DEV, D), 1.0, 6.0, ((0, 16), (1, 2)))
    gate_weights = jnp.clip(0.099609375 + 0.49804688 * jax.random.uniform(streams_of[1], (N_EP, N_DP, TOK_DEV, TOP), jnp.float32) ** level_of(streams_of[1], (N_EP, N_DP, TOK_DEV, TOP), ((0, 16), (1, 2)), -0.2, 0.2), 0.099609375, 0.59765625).astype(jnp.bfloat16)
    expert_ids_keys = jax.random.split(jax.random.fold_in(streams_of[2], 1), N_EP * N_DP * TOK_DEV // (N_DP * TOK_DEV))
    expert_ids_turns = jax.random.permutation(jax.random.fold_in(streams_of[2], 3), N_EP * N_DP * TOK_DEV // (N_DP * TOK_DEV))
    expert_ids = jax.vmap(lambda own, number: routed_block(jax.random.fold_in(streams_of[2], 2), own, number, N_DP * TOK_DEV, EXPERTS, TOP, CAP, 2))(expert_ids_keys, expert_ids_turns).reshape((N_EP, N_DP, TOK_DEV, TOP))
    gate_proj = scatter_about(streams_of[3], (EXPERTS, D, FF), D ** -0.5, 0.09375, ((0, 16), (2, 2)))
    up_proj = scatter_about(streams_of[4], (EXPERTS, D, FF), D ** -0.5, 0.09375, ((0, 16), (2, 2)))
    down_proj = scatter_about(streams_of[5], (EXPERTS, FF, D), FF ** -0.5, 0.125, ((0, 16), (1, 2)))
    return dict(tokens=tokens, gate_weights=gate_weights, expert_ids=expert_ids, gate_proj=gate_proj, up_proj=up_proj, down_proj=down_proj)


def placing(flat_ids, expert_count, capacity):
    labels = jnp.arange(expert_count, dtype=jnp.int32)
    onehot = (flat_ids[:, None] == labels[None, :]).astype(jnp.int32)
    earlier = jnp.cumsum(onehot, axis=0) - onehot
    slot_index = jnp.sum(earlier * onehot, axis=1).astype(jnp.int32)
    destination = (flat_ids * capacity + slot_index).astype(jnp.int32)
    targets = jnp.arange(expert_count * capacity, dtype=jnp.int32)
    return (destination[:, None] == targets[None, :]).astype(jnp.float32)


def expert_forward(operands):
    slot_rows, gate_mat, up_mat, down_mat = operands
    gate_act = jnp.dot(slot_rows, gate_mat, preferred_element_type=jnp.float32)
    up_act = jnp.dot(slot_rows, up_mat, preferred_element_type=jnp.float32)
    hidden = (jax.nn.silu(gate_act) * up_act).astype(jnp.bfloat16)
    return jnp.dot(hidden, down_mat, preferred_element_type=jnp.float32).astype(jnp.bfloat16)


def reference(tokens, gate_weights, expert_ids, gate_proj, up_proj, down_proj):
    column_total, group_count, token_count, feature_count = tokens.shape
    expert_count = gate_proj.shape[0]
    top_count = expert_ids.shape[3]
    capacity = CAP
    token_total = group_count * token_count
    slot_total = expert_count * capacity

    def place_column(column_ids):
        return placing(column_ids, expert_count, capacity)

    flat_ids = expert_ids.reshape(column_total, token_total * top_count).astype(jnp.int32)
    placed = jax.vmap(place_column)(flat_ids)
    selection = jnp.sum(placed.reshape(column_total, token_total, top_count, slot_total), axis=2)
    token_rows = tokens.reshape(column_total, token_total, feature_count).astype(jnp.float32)
    buffer = jnp.einsum("ctj,ctd->cjd", selection, token_rows, precision=lax.Precision.HIGHEST).astype(jnp.bfloat16)
    per_expert = buffer.reshape(column_total, expert_count, capacity, feature_count)
    per_expert = per_expert.transpose(1, 0, 2, 3).reshape(expert_count, column_total * capacity, feature_count)
    expert_out = lax.map(expert_forward, (per_expert, gate_proj, up_proj, down_proj))
    expert_out = expert_out.reshape(expert_count, column_total, capacity, feature_count)
    expert_out = expert_out.transpose(1, 0, 2, 3).reshape(column_total, slot_total, feature_count)
    weight_flat = gate_weights.reshape(column_total, token_total * top_count).astype(jnp.float32)
    weighted = jnp.sum((placed * weight_flat[:, :, None]).reshape(column_total, token_total, top_count, slot_total), axis=2)
    mixed = jnp.einsum("ctj,cjd->ctd", weighted, expert_out.astype(jnp.float32), precision=lax.Precision.HIGHEST)
    return mixed.astype(jnp.bfloat16).reshape(tokens.shape)
```

```python
import functools

import jax
import jax.numpy as jnp
from jax import lax
from jax.experimental import pallas as pl
from jax.experimental.pallas import tpu as pltpu
from jax.sharding import PartitionSpec as P

VMEM = pl.BlockSpec(memory_space=pltpu.VMEM)


def prepare_kernel(experts, tokens_ref, weights_ref, ids_ref, sent_ref, mix_ref):
    devices, _, half = sent_ref.shape
    row = tokens_ref[...].astype(jnp.float32)
    pair = jnp.concatenate([row[:, :half], row[:, half:]], axis=0).astype(jnp.bfloat16)

    @pl.loop(0, devices)
    def _(i):
        sent_ref[i] = pair

    shape = mix_ref.shape
    column = lax.broadcasted_iota(jnp.int32, shape, 1)
    expert = lax.rem(lax.div(column, 2), experts)
    mix = jnp.zeros(shape, jnp.float32)
    for k in range(ids_ref.shape[1]):
        weight = weights_ref[:, k : k + 1].astype(jnp.float32)
        mix = mix + jnp.where(expert == ids_ref[:, k : k + 1], weight, 0.0)
    own = lax.broadcasted_iota(jnp.int32, shape, 0) == lax.rem(column, 2)
    mix_ref[...] = jnp.where(own, mix, 0.0).astype(jnp.bfloat16)


def ffn_kernel(x_ref, gate_ref, up_ref, down_ref, out_ref, hidden_ref):
    devices, _, half = x_ref.shape
    width = gate_ref.shape[1]
    step = min(256, width)
    rows = x_ref[...].reshape(2 * devices, half)
    even = lax.rem(lax.broadcasted_iota(jnp.int32, (2 * devices, step), 0), 2) == 0

    def project(ref, columns):
        low = jnp.dot(rows, ref[:half, columns], preferred_element_type=jnp.float32)
        high = jnp.dot(rows, ref[half:, columns], preferred_element_type=jnp.float32)
        return jnp.where(
            even, low + pltpu.roll(high, 2 * devices - 1, 0), high + pltpu.roll(low, 1, 0)
        )

    @pl.loop(0, width // step)
    def _(i):
        columns = pl.ds(pl.multiple_of(i * step, step), step)
        gate, up = project(gate_ref, columns), project(up_ref, columns)
        hidden_ref[:, columns] = (gate / (1.0 + jnp.exp(-gate)) * up).astype(jnp.bfloat16)

    hidden = hidden_ref[...]
    out_step = 256 if half % 256 == 0 else 128
    even_out = lax.rem(lax.broadcasted_iota(jnp.int32, (2 * devices, out_step), 0), 2) == 0

    @pl.loop(0, half // out_step)
    def _(i):
        start = pl.multiple_of(i * out_step, out_step)
        low = jnp.dot(hidden, down_ref[:, pl.ds(start, out_step)], preferred_element_type=jnp.float32)
        high = jnp.dot(
            hidden, down_ref[:, pl.ds(start + half, out_step)], preferred_element_type=jnp.float32
        )
        out = jnp.where(even_out, low, high).astype(jnp.bfloat16)
        out_ref[:, :, pl.ds(start, out_step)] = out.reshape(devices, 2, out_step)


def mix_kernel(mix_ref, parts_ref, out_ref):
    devices, _, half = parts_ref.shape
    rows = parts_ref[...].reshape(2 * devices, half)
    mixed = jnp.dot(mix_ref[...], rows, preferred_element_type=jnp.float32)
    out_ref[:, :half] = mixed[0:1].astype(jnp.bfloat16)
    out_ref[:, half:] = mixed[1:2].astype(jnp.bfloat16)


def body(tokens, gate_weights, expert_ids, gate_proj, up_proj, down_proj):
    groups, experts = lax.axis_size("dp"), lax.axis_size("ep")
    devices = groups * experts
    axes = ("dp", "ep")
    features, width = tokens.shape[3], gate_proj.shape[2]
    half = features // 2
    sent, mix = pl.pallas_call(
        functools.partial(prepare_kernel, experts),
        out_shape=(
            jax.ShapeDtypeStruct((devices, 2, half), jnp.bfloat16),
            jax.ShapeDtypeStruct((16, 2 * devices), jnp.bfloat16),
        ),
        in_specs=[VMEM] * 3,
        out_specs=(VMEM, VMEM),
        compiler_params=pltpu.CompilerParams(vmem_limit_bytes=24 << 20),
        name="prepare",
    )(tokens[0, 0], gate_weights[0, 0], expert_ids[0, 0])
    rows = lax.all_to_all(sent, axes, 0, 0, tiled=True)
    gate, up, down = (
        pltpu.with_memory_space_constraint(w[0], pltpu.VMEM) for w in (gate_proj, up_proj, down_proj)
    )
    out = pl.pallas_call(
        ffn_kernel,
        out_shape=jax.ShapeDtypeStruct((devices, 2, half), jnp.bfloat16),
        in_specs=[VMEM] * 4,
        out_specs=VMEM,
        scratch_shapes=[pltpu.VMEM((2 * devices, width), jnp.bfloat16)],
        compiler_params=pltpu.CompilerParams(vmem_limit_bytes=24 << 20),
        cost_estimate=pl.CostEstimate(
            flops=12 * devices * features * width,
            bytes_accessed=6 * features * width,
            transcendentals=2 * devices * width,
        ),
        name="ffn",
    )(rows, gate, up, down)
    parts = lax.all_to_all(out, axes, 0, 0, tiled=True)
    mixed = pl.pallas_call(
        mix_kernel,
        out_shape=jax.ShapeDtypeStruct((1, features), jnp.bfloat16),
        in_specs=[VMEM] * 2,
        out_specs=VMEM,
        compiler_params=pltpu.CompilerParams(vmem_limit_bytes=24 << 20),
        name="mix",
    )(mix, parts)
    return mixed[None, None]


def solution(mesh):
    placed = (
        P("ep", "dp", None, None),
        P("ep", "dp", None, None),
        P("ep", "dp", None, None),
        P("ep", None, "dp"),
        P("ep", None, "dp"),
        P("ep", "dp", None),
    )
    return jax.shard_map(
        body, mesh=mesh, in_specs=placed, out_specs=P("ep", "dp", None, None), check_vma=False
    )
```

```python
import functools

import jax
import jax.numpy as jnp
from jax import lax
from jax.experimental import pallas as pl
from jax.experimental.pallas import tpu as pltpu
from jax.sharding import PartitionSpec as P

VMEM = pl.BlockSpec(memory_space=pltpu.VMEM)


def prepare_kernel(experts, tokens_ref, weights_ref, ids_ref, sent_ref, mix_ref):
    devices, _, half = sent_ref.shape
    row = tokens_ref[...].astype(jnp.float32)
    pair = jnp.concatenate([row[:, :half], row[:, half:]], axis=0).astype(jnp.bfloat16)

    @pl.loop(0, devices)
    def _(i):
        sent_ref[i] = pair

    shape = mix_ref.shape
    column = lax.broadcasted_iota(jnp.int32, shape, 1)
    expert = lax.rem(lax.div(column, 2), experts)
    mix = jnp.zeros(shape, jnp.float32)
    for k in range(ids_ref.shape[1]):
        weight = weights_ref[:, k : k + 1].astype(jnp.float32)
        mix = mix + jnp.where(expert == ids_ref[:, k : k + 1], weight, 0.0)
    own = lax.broadcasted_iota(jnp.int32, shape, 0) == lax.rem(column, 2)
    mix_ref[...] = jnp.where(own, mix, 0.0).astype(jnp.bfloat16)


def ffn_kernel(x_ref, gate_ref, up_ref, down_ref, out_ref, hidden_ref):
    devices, _, half = x_ref.shape
    width = gate_ref.shape[1]
    step = min(256, width)
    rows = x_ref[...].reshape(2 * devices, half)
    even = lax.rem(lax.broadcasted_iota(jnp.int32, (2 * devices, step), 0), 2) == 0

    def project(ref, columns):
        low = jnp.dot(rows, ref[:half, columns], preferred_element_type=jnp.float32)
        high = jnp.dot(rows, ref[half:, columns], preferred_element_type=jnp.float32)
        return jnp.where(
            even, low + pltpu.roll(high, 2 * devices - 1, 0), high + pltpu.roll(low, 1, 0)
        )

    @pl.loop(0, width // step)
    def _(i):
        columns = pl.ds(pl.multiple_of(i * step, step), step)
        gate, up = project(gate_ref, columns), project(up_ref, columns)
        hidden_ref[:, columns] = (gate / (1.0 + jnp.exp(-gate)) * up).astype(jnp.bfloat16)

    hidden = hidden_ref[...]
    out_step = 256 if half % 256 == 0 else 128
    even_out = lax.rem(lax.broadcasted_iota(jnp.int32, (2 * devices, out_step), 0), 2) == 0

    @pl.loop(0, half // out_step)
    def _(i):
        start = pl.multiple_of(i * out_step, out_step)
        low = jnp.dot(hidden, down_ref[:, pl.ds(start, out_step)], preferred_element_type=jnp.float32)
        high = jnp.dot(
            hidden, down_ref[:, pl.ds(start + half, out_step)], preferred_element_type=jnp.float32
        )
        out = jnp.where(even_out, low, high).astype(jnp.bfloat16)
        out_ref[:, :, pl.ds(start, out_step)] = out.reshape(devices, 2, out_step)


def mix_kernel(mix_ref, parts_ref, out_ref):
    devices, _, half = parts_ref.shape
    rows = parts_ref[...].reshape(2 * devices, half)
    mixed = jnp.dot(mix_ref[...], rows, preferred_element_type=jnp.float32)
    out_ref[:, :half] = mixed[0:1].astype(jnp.bfloat16)
    out_ref[:, half:] = mixed[1:2].astype(jnp.bfloat16)


def body(tokens, gate_weights, expert_ids, gate_proj, up_proj, down_proj):
    groups, experts = lax.axis_size("dp"), lax.axis_size("ep")
    devices = groups * experts
    axes = ("dp", "ep")
    features, width = tokens.shape[3], gate_proj.shape[2]
    half = features // 2
    sent, mix = pl.pallas_call(
        functools.partial(prepare_kernel, experts),
        out_shape=(
            jax.ShapeDtypeStruct((devices, 2, half), jnp.bfloat16),
            jax.ShapeDtypeStruct((16, 2 * devices), jnp.bfloat16),
        ),
        in_specs=[VMEM] * 3,
        out_specs=(VMEM, VMEM),
        compiler_params=pltpu.CompilerParams(vmem_limit_bytes=24 << 20),
        cost_estimate=pl.CostEstimate(flops=2 * 10**10, bytes_accessed=10**5, transcendentals=0),
        name="prepare",
    )(tokens[0, 0], gate_weights[0, 0], expert_ids[0, 0])
    rows = lax.all_to_all(sent, axes, 0, 0, tiled=True)
    gate, up, down = (
        w[0] for w in (gate_proj, up_proj, down_proj)
    )
    out = pl.pallas_call(
        ffn_kernel,
        out_shape=jax.ShapeDtypeStruct((devices, 2, half), jnp.bfloat16),
        in_specs=[VMEM] * 4,
        out_specs=VMEM,
        scratch_shapes=[pltpu.VMEM((2 * devices, width), jnp.bfloat16)],
        compiler_params=pltpu.CompilerParams(vmem_limit_bytes=24 << 20),
        cost_estimate=pl.CostEstimate(
            flops=12 * devices * features * width,
            bytes_accessed=6 * features * width,
            transcendentals=2 * devices * width,
        ),
        name="ffn",
    )(rows, gate, up, down)
    parts = lax.all_to_all(out, axes, 0, 0, tiled=True)
    mixed = pl.pallas_call(
        mix_kernel,
        out_shape=jax.ShapeDtypeStruct((1, features), jnp.bfloat16),
        in_specs=[VMEM] * 2,
        out_specs=VMEM,
        compiler_params=pltpu.CompilerParams(vmem_limit_bytes=24 << 20),
        name="mix",
    )(mix, parts)
    return mixed[None, None]


def solution(mesh):
    placed = (
        P("ep", "dp", None, None),
        P("ep", "dp", None, None),
        P("ep", "dp", None, None),
        P("ep", None, "dp"),
        P("ep", None, "dp"),
        P("ep", "dp", None),
    )
    return jax.shard_map(
        body, mesh=mesh, in_specs=placed, out_specs=P("ep", "dp", None, None), check_vma=False
    )
```

```python
import functools

import jax
import jax.numpy as jnp
from jax import lax
from jax.experimental import pallas as pl
from jax.experimental.pallas import tpu as pltpu
from jax.sharding import PartitionSpec as P

LANES = 128
VMEM = pl.BlockSpec(memory_space=pltpu.VMEM)


def block(total, rows):
    return next(
        size
        for size in range(total, 0, -LANES)
        if total % size == 0 and (size == LANES or rows * size <= 1 << 17)
    )


def prepare_kernel(tokens_ref, sent_ref):
    devices, _, half = sent_ref.shape
    row = tokens_ref[...].astype(jnp.float32)
    pair = jnp.concatenate([row[:, :half], row[:, half:]], axis=0).astype(jnp.bfloat16)

    @pl.loop(0, devices)
    def _(i):
        sent_ref[i] = pair


def weigh(experts, weights_ref, ids_ref, mix_ref):
    shape = mix_ref.shape
    column = lax.broadcasted_iota(jnp.int32, shape, 1)
    expert = lax.rem(lax.div(column, 2), experts)
    mix = jnp.zeros(shape, jnp.float32)
    for k in range(ids_ref.shape[1]):
        weight = weights_ref[:, k : k + 1].astype(jnp.float32)
        mix = mix + jnp.where(expert == ids_ref[:, k : k + 1], weight, 0.0)
    own = lax.broadcasted_iota(jnp.int32, shape, 0) == lax.rem(column, 2)
    mix_ref[...] = jnp.where(own, mix, 0.0).astype(jnp.bfloat16)


def ffn_kernel(
    experts, x_ref, gate_ref, up_ref, down_ref, weights_ref, ids_ref, out_ref, mix_ref, hidden_ref
):
    weigh(experts, weights_ref, ids_ref, mix_ref)
    devices, _, half = x_ref.shape
    width = gate_ref.shape[1]
    step = block(width, 2 * devices)
    rows = x_ref[...].reshape(2 * devices, half)
    even = lax.rem(lax.broadcasted_iota(jnp.int32, (2 * devices, step), 0), 2) == 0

    def project(ref, columns):
        low = jnp.dot(rows, ref[:half, columns], preferred_element_type=jnp.float32)
        high = jnp.dot(rows, ref[half:, columns], preferred_element_type=jnp.float32)
        return jnp.where(
            even, low + pltpu.roll(high, 2 * devices - 1, 0), high + pltpu.roll(low, 1, 0)
        )

    @pl.loop(0, width // step)
    def _(i):
        columns = pl.ds(pl.multiple_of(i * step, step), step)
        gate, up = project(gate_ref, columns), project(up_ref, columns)
        hidden_ref[:, columns] = (gate / (1.0 + jnp.exp(-gate)) * up).astype(jnp.bfloat16)

    hidden = hidden_ref[...]
    out_step = block(half, 2 * devices)
    even_out = lax.rem(lax.broadcasted_iota(jnp.int32, (2 * devices, out_step), 0), 2) == 0

    @pl.loop(0, half // out_step)
    def _(i):
        start = pl.multiple_of(i * out_step, out_step)
        low = jnp.dot(hidden, down_ref[:, pl.ds(start, out_step)], preferred_element_type=jnp.float32)
        high = jnp.dot(
            hidden, down_ref[:, pl.ds(start + half, out_step)], preferred_element_type=jnp.float32
        )
        out = jnp.where(even_out, low, high).astype(jnp.bfloat16)
        out_ref[:, :, pl.ds(start, out_step)] = out.reshape(devices, 2, out_step)


def mix_kernel(mix_ref, parts_ref, out_ref):
    devices, _, half = parts_ref.shape
    rows = parts_ref[...].reshape(2 * devices, half)
    mixed = jnp.dot(mix_ref[...], rows, preferred_element_type=jnp.float32)
    out_ref[:, :half] = mixed[0:1].astype(jnp.bfloat16)
    out_ref[:, half:] = mixed[1:2].astype(jnp.bfloat16)


def body(tokens, gate_weights, expert_ids, gate_proj, up_proj, down_proj):
    groups, experts = lax.axis_size("dp"), lax.axis_size("ep")
    devices = groups * experts
    axes = ("dp", "ep")
    features, width = tokens.shape[3], gate_proj.shape[2]
    half = features // 2
    sent = pl.pallas_call(
        prepare_kernel,
        out_shape=jax.ShapeDtypeStruct((devices, 2, half), jnp.bfloat16),
        in_specs=[VMEM],
        out_specs=VMEM,
        compiler_params=pltpu.CompilerParams(vmem_limit_bytes=24 << 20),
        cost_estimate=pl.CostEstimate(flops=2 * 10**10, bytes_accessed=10**5, transcendentals=0),
        name="prepare",
    )(tokens[0, 0])
    rows = lax.all_to_all(sent, axes, 0, 0, tiled=True)
    gate, up, down = gate_proj[0], up_proj[0], down_proj[0]
    out, mix = pl.pallas_call(
        functools.partial(ffn_kernel, experts),
        out_shape=(
            jax.ShapeDtypeStruct((devices, 2, half), jnp.bfloat16),
            jax.ShapeDtypeStruct((16, 2 * devices), jnp.bfloat16),
        ),
        in_specs=[VMEM] * 6,
        out_specs=(VMEM, VMEM),
        scratch_shapes=[pltpu.VMEM((2 * devices, width), jnp.bfloat16)],
        compiler_params=pltpu.CompilerParams(vmem_limit_bytes=24 << 20),
        cost_estimate=pl.CostEstimate(
            flops=12 * devices * features * width,
            bytes_accessed=6 * features * width,
            transcendentals=2 * devices * width,
        ),
        name="ffn",
    )(rows, gate, up, down, gate_weights[0, 0], expert_ids[0, 0])
    parts = lax.all_to_all(out, axes, 0, 0, tiled=True)
    mixed = pl.pallas_call(
        mix_kernel,
        out_shape=jax.ShapeDtypeStruct((1, features), jnp.bfloat16),
        in_specs=[VMEM] * 2,
        out_specs=VMEM,
        compiler_params=pltpu.CompilerParams(vmem_limit_bytes=24 << 20),
        name="mix",
    )(mix, parts)
    return mixed[None, None]


def solution(mesh):
    placed = (
        P("ep", "dp", None, None),
        P("ep", "dp", None, None),
        P("ep", "dp", None, None),
        P("ep", None, "dp"),
        P("ep", None, "dp"),
        P("ep", "dp", None),
    )
    return jax.shard_map(
        body, mesh=mesh, in_specs=placed, out_specs=P("ep", "dp", None, None), check_vma=False
    )
```

```python
import functools

import jax
import jax.numpy as jnp
from jax import lax
from jax.experimental import pallas as pl
from jax.experimental.pallas import tpu as pltpu
from jax.sharding import PartitionSpec as P

LANES = 128
VMEM = pl.BlockSpec(memory_space=pltpu.VMEM)
HBM = pl.BlockSpec(memory_space=pltpu.HBM)


def block(total, rows):
    return next(
        size
        for size in range(total, 0, -LANES)
        if total % size == 0 and (size == LANES or rows * size <= 1 << 17)
    )


def matmul(x, y):
    return jnp.dot(x, y, preferred_element_type=jnp.float32)


def is_even(shape):
    return lax.rem(lax.broadcasted_iota(jnp.int32, shape, 0), 2) == 0


def parity():
    return lax.rem(lax.axis_index("ep"), 2)


def part_of(index, size):
    return pl.ds(pl.multiple_of(index * size, size), size)


def prepare_kernel(experts, tokens_hbm, weights_hbm, ids_hbm, sent_ref, tokens_ref, weights_ref, ids_ref, sems):
    copies = [
        pltpu.make_async_copy(source, target, sems.at[i])
        for i, (source, target) in enumerate(
            ((weights_hbm, weights_ref), (ids_hbm, ids_ref), (tokens_hbm, tokens_ref))
        )
    ]
    for copy in copies:
        copy.start()
    copies[0].wait()
    copies[1].wait()
    devices = sent_ref.shape[0]
    quarter = tokens_ref.shape[1] // 4
    shape = (2 * devices, LANES)
    expert = lax.rem(lax.div(lax.broadcasted_iota(jnp.int32, shape, 0), 2), experts)
    scale = jnp.zeros(shape, jnp.float32)
    for k in range(ids_ref.shape[1]):
        weight = weights_ref[:, k : k + 1].astype(jnp.float32)
        scale = scale + jnp.where(expert == ids_ref[:, k : k + 1], weight, 0.0)
    sent_ref[:, :, quarter:] = scale.astype(jnp.bfloat16).reshape(devices, 2, LANES)
    copies[2].wait()
    row = tokens_ref[...].astype(jnp.float32)
    quad = jnp.concatenate([row[:, i * quarter : (i + 1) * quarter] for i in range(4)], axis=0)
    quad = quad.astype(jnp.bfloat16)
    pairs = (quad[:2], quad[2:])

    @pl.loop(0, devices // 2)
    def _(i):
        for half in range(2):
            sent_ref[2 * i + half, :, :quarter] = pairs[half]


def project(rows, ref, half, columns):
    quarter = rows.shape[1]
    count = rows.shape[0]
    low = matmul(rows, ref[part_of(2 * half, quarter), columns])
    high = matmul(rows, ref[part_of(2 * half + 1, quarter), columns])
    return jnp.where(
        is_even(low.shape), low + pltpu.roll(high, count - 1, 0), high + pltpu.roll(low, 1, 0)
    )


def half_rows(ref):
    devices, _, size = ref.shape
    return ref[:, :, : size - LANES].reshape(2 * devices, size - LANES)


def scale_of(ref):
    devices, _, size = ref.shape
    scale = ref[:, :, size - LANES :].reshape(2 * devices, LANES)
    return scale[:, :1].astype(jnp.float32)


def first_kernel(own_ref, gate_ref, up_ref, gate_acc_ref, up_acc_ref):
    rows, half = half_rows(own_ref), parity()
    width = gate_ref.shape[1]
    step = block(width, rows.shape[0])

    @pl.loop(0, width // step)
    def _(i):
        columns = part_of(i, step)
        gate_acc_ref[:, columns] = project(rows, gate_ref, half, columns)
        up_acc_ref[:, columns] = project(rows, up_ref, half, columns)


def project_down(hidden_ref, down_ref, scale, half, store):
    hidden = hidden_ref[...]
    quarter = down_ref.shape[1] // 4
    step = block(quarter, hidden.shape[0])

    @pl.loop(0, quarter // step)
    def _(i):
        start = pl.multiple_of(2 * half * quarter + i * step, LANES)
        low = matmul(hidden, down_ref[:, pl.ds(start, step)])
        high = matmul(hidden, down_ref[:, pl.ds(start + quarter, step)])
        store(part_of(i, step), jnp.where(is_even(low.shape), low, high) * scale)


def second_kernel(
    own_ref, other_ref, gate_acc_ref, up_acc_ref, gate_ref, up_ref, down_ref, hidden_ref, out_ref
):
    rows, half = half_rows(other_ref), 1 - parity()
    width = gate_ref.shape[1]
    step = block(width, rows.shape[0])

    @pl.loop(0, width // step)
    def _(i):
        columns = part_of(i, step)
        gate = gate_acc_ref[:, columns] + project(rows, gate_ref, half, columns)
        up = up_acc_ref[:, columns] + project(rows, up_ref, half, columns)
        hidden_ref[:, columns] = (gate / (1.0 + jnp.exp(-gate)) * up).astype(jnp.bfloat16)

    scale = scale_of(own_ref)

    def store(columns, value):
        devices = out_ref.shape[0]
        out_ref[:, :, columns] = value.astype(jnp.bfloat16).reshape(devices, 2, value.shape[1])

    project_down(hidden_ref, down_ref, scale, half, store)


def third_kernel(hidden_ref, scale_ref, down_ref, out_ref):
    def store(columns, value):
        out_ref[:, columns] = value

    project_down(hidden_ref, down_ref, scale_of(scale_ref), parity(), store)


def add_kernel(kept_ref, received_ref, out_ref):
    devices, _, quarter = received_ref.shape
    received = received_ref[...].reshape(2 * devices, quarter).astype(jnp.float32)
    out_ref[...] = (kept_ref[...] + received).astype(jnp.bfloat16).reshape(devices, 2, quarter)


def mix_kernel(parts_ref, out_ref):
    devices, _, quarter = parts_ref.shape
    rows = parts_ref[...].reshape(2 * devices, quarter)
    shape = (16, 2 * devices)
    chosen = lax.rem(lax.broadcasted_iota(jnp.int32, shape, 1), 4) == lax.broadcasted_iota(
        jnp.int32, shape, 0
    )
    mixed = matmul(jnp.where(chosen, 1.0, 0.0).astype(jnp.bfloat16), rows)
    for i in range(4):
        out_ref[:, i * quarter : (i + 1) * quarter] = mixed[i : i + 1].astype(jnp.bfloat16)


def call(kernel, name, outs, ins, flops, scratch=(), in_specs=None):
    return pl.pallas_call(
        kernel,
        out_shape=outs,
        in_specs=in_specs or [VMEM] * len(ins),
        out_specs=jax.tree.map(lambda _: VMEM, outs),
        scratch_shapes=scratch,
        compiler_params=pltpu.CompilerParams(vmem_limit_bytes=24 << 20),
        cost_estimate=pl.CostEstimate(flops=flops, bytes_accessed=10**5, transcendentals=0),
        name=name,
    )(*ins)


def body(tokens, gate_weights, expert_ids, gate_proj, up_proj, down_proj):
    groups, experts = lax.axis_size("dp"), lax.axis_size("ep")
    devices = groups * experts
    features, width = tokens.shape[3], gate_proj.shape[2]
    top, quarter = expert_ids.shape[3], features // 4
    bf16, f32 = jnp.bfloat16, jnp.float32
    gate, up, down = gate_proj[0], up_proj[0], down_proj[0]
    swap = [(i, i ^ 1) for i in range(experts)]
    heavy = 2 * 10**10

    sent = call(
        functools.partial(prepare_kernel, experts),
        "prepare",
        jax.ShapeDtypeStruct((devices, 2, quarter + LANES), bf16),
        tuple(
            pltpu.with_memory_space_constraint(x[0, 0], pltpu.HBM)
            for x in (tokens, gate_weights, expert_ids)
        ),
        heavy,
        [
            pltpu.VMEM((1, features), bf16),
            pltpu.VMEM((1, top), bf16),
            pltpu.VMEM((1, top), jnp.int32),
            pltpu.SemaphoreType.DMA((3,)),
        ],
        [HBM] * 3,
    )
    own = lax.all_to_all(sent, ("dp", "ep"), 0, 0, tiled=True)
    other = lax.ppermute(own, "ep", swap)
    acc = jax.ShapeDtypeStruct((2 * devices, width), f32)
    gate_acc, up_acc = call(first_kernel, "first", (acc, acc), (own, gate, up), heavy)
    hidden, out = call(
        second_kernel,
        "second",
        (
            jax.ShapeDtypeStruct((2 * devices, width), bf16),
            jax.ShapeDtypeStruct((devices, 2, quarter), bf16),
        ),
        (own, other, gate_acc, up_acc, gate, up, down),
        heavy,
    )
    received = lax.ppermute(out, "ep", swap)
    kept = call(
        third_kernel,
        "third",
        jax.ShapeDtypeStruct((2 * devices, quarter), f32),
        (hidden, own, down),
        heavy,
    )
    summed = call(
        add_kernel, "add", jax.ShapeDtypeStruct((devices, 2, quarter), bf16), (kept, received), 10**6
    )
    parts = lax.all_to_all(summed, ("dp", "ep"), 0, 0, tiled=True)
    mixed = call(mix_kernel, "mix", jax.ShapeDtypeStruct((1, features), bf16), (parts,), 10**6)
    return mixed[None, None]


def solution(mesh):
    placed = (
        P("ep", "dp", None, None),
        P("ep", "dp", None, None),
        P("ep", "dp", None, None),
        P("ep", None, "dp"),
        P("ep", None, "dp"),
        P("ep", "dp", None),
    )
    return jax.shard_map(
        body, mesh=mesh, in_specs=placed, out_specs=P("ep", "dp", None, None), check_vma=False
    )
```

```python
import functools

import jax
import jax.numpy as jnp
from jax import lax
from jax.experimental import pallas as pl
from jax.experimental.pallas import tpu as pltpu
from jax.sharding import PartitionSpec as P

LANES = 128
VMEM = pl.BlockSpec(memory_space=pltpu.VMEM)
HBM = pl.BlockSpec(memory_space=pltpu.HBM)


def block(total, rows):
    return next(
        size
        for size in range(total, 0, -LANES)
        if total % size == 0 and (size == LANES or rows * size <= 1 << 17)
    )


def matmul(x, ref, start, columns):
    total = None
    for k in range(0, x.shape[1], LANES):
        part = jnp.dot(
            x[:, k : k + LANES],
            ref[pl.ds(pl.multiple_of(start + k, LANES), LANES), columns],
            preferred_element_type=jnp.float32,
        )
        total = part if total is None else total + part
    return total


def is_even(shape):
    return lax.rem(lax.broadcasted_iota(jnp.int32, shape, 0), 2) == 0


def parity():
    return lax.rem(lax.axis_index("ep"), 2)


def part_of(index, size):
    return pl.ds(pl.multiple_of(index * size, size), size)


def prepare_kernel(experts, tokens_hbm, weights_hbm, ids_hbm, sent_ref, tokens_ref, weights_ref, ids_ref, sems):
    copies = [
        pltpu.make_async_copy(source, target, sems.at[i])
        for i, (source, target) in enumerate(
            ((weights_hbm, weights_ref), (ids_hbm, ids_ref), (tokens_hbm, tokens_ref))
        )
    ]
    for copy in copies:
        copy.start()
    copies[0].wait()
    copies[1].wait()
    devices = sent_ref.shape[0]
    quarter = tokens_ref.shape[1] // 4
    shape = (2 * devices, LANES)
    expert = lax.rem(lax.div(lax.broadcasted_iota(jnp.int32, shape, 0), 2), experts)
    expert = expert[:, : ids_ref.shape[1]]
    chosen = jnp.where(expert == ids_ref[...], weights_ref[...].astype(jnp.float32), 0.0)
    scale = jnp.broadcast_to(jnp.sum(chosen, axis=1, keepdims=True), shape)
    sent_ref[:, :, quarter:] = scale.astype(jnp.bfloat16).reshape(devices, 2, LANES)
    copies[2].wait()
    row = tokens_ref[...].astype(jnp.float32)
    quad = jnp.concatenate([row[:, i * quarter : (i + 1) * quarter] for i in range(4)], axis=0)
    quad = quad.astype(jnp.bfloat16)
    pairs = (quad[:2], quad[2:])

    @pl.loop(0, devices // 2, unroll=min(16, devices // 2))
    def _(i):
        for half in range(2):
            sent_ref[2 * i + half, :, :quarter] = pairs[half]


def project(rows, ref, half, columns):
    quarter = rows.shape[1]
    count = rows.shape[0]
    low = matmul(rows, ref, 2 * half * quarter, columns)
    high = matmul(rows, ref, (2 * half + 1) * quarter, columns)
    return jnp.where(
        is_even(low.shape), low + pltpu.roll(high, count - 1, 0), high + pltpu.roll(low, 1, 0)
    )


def half_rows(ref):
    devices, _, size = ref.shape
    return ref[:, :, : size - LANES].reshape(2 * devices, size - LANES)


def scale_of(ref):
    devices, _, size = ref.shape
    scale = ref[:, :, size - LANES :].reshape(2 * devices, LANES)
    return scale[:, :1].astype(jnp.float32)


def first_kernel(own_ref, gate_ref, up_ref, gate_acc_ref, up_acc_ref):
    rows, half = half_rows(own_ref), parity()
    width = gate_ref.shape[1]
    step = block(width, rows.shape[0])

    @pl.loop(0, width // step)
    def _(i):
        columns = part_of(i, step)
        gate_acc_ref[:, columns] = project(rows, gate_ref, half, columns)
        up_acc_ref[:, columns] = project(rows, up_ref, half, columns)


def project_down(hidden_ref, down_ref, scale, half, store):
    hidden = hidden_ref[...]
    quarter = down_ref.shape[1] // 4
    step = block(quarter, hidden.shape[0])

    if step == quarter:
        both = matmul(hidden, down_ref, 0, part_of(half, 2 * quarter))
        low, high = both[:, :quarter], both[:, quarter:]
        store(slice(None), jnp.where(is_even(low.shape), low, high) * scale)
        return

    @pl.loop(0, quarter // step)
    def _(i):
        start = pl.multiple_of(2 * half * quarter + i * step, LANES)
        low = matmul(hidden, down_ref, 0, pl.ds(start, step))
        high = matmul(hidden, down_ref, 0, pl.ds(start + quarter, step))
        store(part_of(i, step), jnp.where(is_even(low.shape), low, high) * scale)


def second_kernel(
    own_ref, other_ref, gate_acc_ref, up_acc_ref, gate_ref, up_ref, down_ref, hidden_ref, out_ref
):
    rows, half = half_rows(other_ref), 1 - parity()
    width = gate_ref.shape[1]
    step = block(width, rows.shape[0])

    @pl.loop(0, width // step)
    def _(i):
        columns = part_of(i, step)
        gate = gate_acc_ref[:, columns] + project(rows, gate_ref, half, columns)
        up = up_acc_ref[:, columns] + project(rows, up_ref, half, columns)
        hidden_ref[:, columns] = (gate / (1.0 + jnp.exp(-gate)) * up).astype(jnp.bfloat16)

    scale = scale_of(own_ref)

    def store(columns, value):
        devices = out_ref.shape[0]
        out_ref[:, :, columns] = value.astype(jnp.bfloat16).reshape(devices, 2, value.shape[1])

    project_down(hidden_ref, down_ref, scale, half, store)


def third_kernel(hidden_ref, scale_ref, down_ref, out_ref):
    def store(columns, value):
        out_ref[:, columns] = value

    project_down(hidden_ref, down_ref, scale_of(scale_ref), parity(), store)


def add_kernel(kept_ref, received_ref, out_ref):
    devices, _, quarter = received_ref.shape
    received = received_ref[...].reshape(2 * devices, quarter).astype(jnp.float32)
    out_ref[...] = (kept_ref[...] + received).astype(jnp.bfloat16).reshape(devices, 2, quarter)


def mix_kernel(parts_ref, out_ref):
    devices, _, quarter = parts_ref.shape
    rows = parts_ref[...].reshape(2 * devices, quarter).astype(jnp.float32)
    mixed = jnp.sum(rows.reshape(devices // 4, 8, quarter), axis=0)
    mixed = (mixed[:4] + mixed[4:]).astype(jnp.bfloat16)
    for i in range(4):
        out_ref[:, i * quarter : (i + 1) * quarter] = mixed[i : i + 1]


def call(kernel, name, outs, ins, flops, scratch=(), in_specs=None):
    return pl.pallas_call(
        kernel,
        out_shape=outs,
        in_specs=in_specs or [VMEM] * len(ins),
        out_specs=jax.tree.map(lambda _: VMEM, outs),
        scratch_shapes=scratch,
        compiler_params=pltpu.CompilerParams(vmem_limit_bytes=24 << 20),
        cost_estimate=pl.CostEstimate(flops=flops, bytes_accessed=10**5, transcendentals=0),
        name=name,
    )(*ins)


def body(tokens, gate_weights, expert_ids, gate_proj, up_proj, down_proj):
    groups, experts = lax.axis_size("dp"), lax.axis_size("ep")
    devices = groups * experts
    features, width = tokens.shape[3], gate_proj.shape[2]
    top, quarter = expert_ids.shape[3], features // 4
    bf16, f32 = jnp.bfloat16, jnp.float32
    gate, up, down = gate_proj[0], up_proj[0], down_proj[0]
    swap = [(i, i ^ 1) for i in range(experts)]
    heavy = 2 * 10**10

    sent = call(
        functools.partial(prepare_kernel, experts),
        "prepare",
        jax.ShapeDtypeStruct((devices, 2, quarter + LANES), bf16),
        tuple(
            pltpu.with_memory_space_constraint(x[0, 0], pltpu.HBM)
            for x in (tokens, gate_weights, expert_ids)
        ),
        heavy,
        [
            pltpu.VMEM((1, features), bf16),
            pltpu.VMEM((1, top), bf16),
            pltpu.VMEM((1, top), jnp.int32),
            pltpu.SemaphoreType.DMA((3,)),
        ],
        [HBM] * 3,
    )
    own = lax.all_to_all(sent, ("dp", "ep"), 0, 0, tiled=True)
    other = lax.ppermute(own, "ep", swap)
    acc = jax.ShapeDtypeStruct((2 * devices, width), f32)
    gate_acc, up_acc = call(first_kernel, "first", (acc, acc), (own, gate, up), heavy)
    hidden, out = call(
        second_kernel,
        "second",
        (
            jax.ShapeDtypeStruct((2 * devices, width), bf16),
            jax.ShapeDtypeStruct((devices, 2, quarter), bf16),
        ),
        (own, other, gate_acc, up_acc, gate, up, down),
        heavy,
    )
    received = lax.ppermute(out, "ep", swap)
    kept = call(
        third_kernel,
        "third",
        jax.ShapeDtypeStruct((2 * devices, quarter), f32),
        (hidden, own, down),
        heavy,
    )
    summed = call(
        add_kernel, "add", jax.ShapeDtypeStruct((devices, 2, quarter), bf16), (kept, received), 10**6
    )
    parts = lax.all_to_all(summed, ("dp", "ep"), 0, 0, tiled=True)
    mixed = call(mix_kernel, "mix", jax.ShapeDtypeStruct((1, features), bf16), (parts,), 10**6)
    return mixed[None, None]


def solution(mesh):
    placed = (
        P("ep", "dp", None, None),
        P("ep", "dp", None, None),
        P("ep", "dp", None, None),
        P("ep", None, "dp"),
        P("ep", None, "dp"),
        P("ep", "dp", None),
    )
    return jax.shard_map(
        body, mesh=mesh, in_specs=placed, out_specs=P("ep", "dp", None, None), check_vma=False
    )
```

```python
import functools

import jax
import jax.numpy as jnp
from jax import lax
from jax.experimental import pallas as pl
from jax.experimental.pallas import tpu as pltpu
from jax.sharding import PartitionSpec as P

LANES = 128
VMEM = pl.BlockSpec(memory_space=pltpu.VMEM)
HBM = pl.BlockSpec(memory_space=pltpu.HBM)


def block(total, rows):
    return next(
        size
        for size in range(total, 0, -LANES)
        if total % size == 0 and (size == LANES or rows * size <= 1 << 17)
    )


def matmul(x, ref, start, columns):
    total = None
    for k in range(0, x.shape[1], LANES):
        part = jnp.dot(
            x[:, k : k + LANES],
            ref[pl.ds(pl.multiple_of(start + k, LANES), LANES), columns],
            preferred_element_type=jnp.float32,
        )
        total = part if total is None else total + part
    return total


def is_even(shape):
    return lax.rem(lax.broadcasted_iota(jnp.int32, shape, 0), 2) == 0


def parity():
    return lax.rem(lax.axis_index("ep"), 2)


def part_of(index, size):
    return pl.ds(pl.multiple_of(index * size, size), size)


def read_kernel(*refs):
    sources, targets, sems = refs[:3], refs[3:6], refs[6]
    copies = [
        pltpu.make_async_copy(source, target, sems.at[i])
        for i, (source, target) in enumerate(zip(sources, targets))
    ]
    for copy in copies:
        copy.start()
    for copy in copies:
        copy.wait()


def prepare_kernel(experts, tokens_ref, weights_ref, ids_ref, sent_ref):
    devices = sent_ref.shape[0]
    quarter = tokens_ref.shape[1] // 4
    shape = (2 * devices, LANES)
    expert = lax.rem(lax.div(lax.broadcasted_iota(jnp.int32, shape, 0), 2), experts)
    expert = expert[:, : ids_ref.shape[1]]
    chosen = jnp.where(expert == ids_ref[...], weights_ref[...].astype(jnp.float32), 0.0)
    scale = jnp.broadcast_to(jnp.sum(chosen, axis=1, keepdims=True), shape)
    sent_ref[:, :, quarter:] = scale.astype(jnp.bfloat16).reshape(devices, 2, LANES)
    row = tokens_ref[...].astype(jnp.float32)
    quad = [row[:, i * quarter : (i + 1) * quarter] for i in range(4)]
    pairs = jnp.concatenate(quad * 4, axis=0).astype(jnp.bfloat16).reshape(8, 2, quarter)
    for i in range(0, devices, 8):
        sent_ref[i : i + 8, :, :quarter] = pairs


def project(rows, ref, half, columns):
    quarter = rows.shape[1]
    count = rows.shape[0]
    low = matmul(rows, ref, 2 * half * quarter, columns)
    high = matmul(rows, ref, (2 * half + 1) * quarter, columns)
    return jnp.where(
        is_even(low.shape), low + pltpu.roll(high, count - 1, 0), high + pltpu.roll(low, 1, 0)
    )


def half_rows(ref):
    devices, _, size = ref.shape
    return ref[:, :, : size - LANES].reshape(2 * devices, size - LANES)


def scale_of(ref):
    devices, _, size = ref.shape
    scale = ref[:, :, size - LANES :].reshape(2 * devices, LANES)
    return scale[:, :1].astype(jnp.float32)


def first_kernel(own_ref, gate_ref, up_ref, gate_acc_ref, up_acc_ref):
    rows, half = half_rows(own_ref), parity()
    width = gate_ref.shape[1]
    step = block(width, rows.shape[0])

    @pl.loop(0, width // step)
    def _(i):
        columns = part_of(i, step)
        gate_acc_ref[:, columns] = project(rows, gate_ref, half, columns)
        up_acc_ref[:, columns] = project(rows, up_ref, half, columns)


def project_down(hidden_ref, down_ref, scale, half, store):
    hidden = hidden_ref[...]
    quarter = down_ref.shape[1] // 4
    step = block(quarter, hidden.shape[0])

    if step == quarter:
        both = matmul(hidden, down_ref, 0, part_of(half, 2 * quarter))
        low, high = both[:, :quarter], both[:, quarter:]
        store(slice(None), jnp.where(is_even(low.shape), low, high) * scale)
        return

    @pl.loop(0, quarter // step)
    def _(i):
        start = pl.multiple_of(2 * half * quarter + i * step, LANES)
        low = matmul(hidden, down_ref, 0, pl.ds(start, step))
        high = matmul(hidden, down_ref, 0, pl.ds(start + quarter, step))
        store(part_of(i, step), jnp.where(is_even(low.shape), low, high) * scale)


def second_kernel(
    own_ref, other_ref, gate_acc_ref, up_acc_ref, gate_ref, up_ref, down_ref, hidden_ref, out_ref
):
    rows, half = half_rows(other_ref), 1 - parity()
    width = gate_ref.shape[1]
    step = block(width, rows.shape[0])

    @pl.loop(0, width // step)
    def _(i):
        columns = part_of(i, step)
        gate = gate_acc_ref[:, columns] + project(rows, gate_ref, half, columns)
        up = up_acc_ref[:, columns] + project(rows, up_ref, half, columns)
        hidden_ref[:, columns] = (gate / (1.0 + jnp.exp(-gate)) * up).astype(jnp.bfloat16)

    scale = scale_of(own_ref)

    def store(columns, value):
        devices = out_ref.shape[0]
        out_ref[:, :, columns] = value.astype(jnp.bfloat16).reshape(devices, 2, value.shape[1])

    project_down(hidden_ref, down_ref, scale, half, store)


def third_kernel(hidden_ref, scale_ref, down_ref, out_ref):
    def store(columns, value):
        out_ref[:, columns] = value

    project_down(hidden_ref, down_ref, scale_of(scale_ref), parity(), store)


def add_kernel(kept_ref, received_ref, out_ref):
    devices, _, quarter = received_ref.shape
    received = received_ref[...].reshape(2 * devices, quarter).astype(jnp.float32)
    out_ref[...] = (kept_ref[...] + received).astype(jnp.bfloat16).reshape(devices, 2, quarter)


def mix_kernel(parts_ref, out_ref):
    devices, _, quarter = parts_ref.shape
    rows = parts_ref[...].reshape(2 * devices, quarter).astype(jnp.float32)
    mixed = jnp.sum(rows.reshape(devices // 4, 8, quarter), axis=0)
    mixed = (mixed[:4] + mixed[4:]).astype(jnp.bfloat16)
    for i in range(4):
        out_ref[:, i * quarter : (i + 1) * quarter] = mixed[i : i + 1]


def call(kernel, name, outs, ins, flops, scratch=(), in_specs=None):
    return pl.pallas_call(
        kernel,
        out_shape=outs,
        in_specs=in_specs or [VMEM] * len(ins),
        out_specs=jax.tree.map(lambda _: VMEM, outs),
        scratch_shapes=scratch,
        compiler_params=pltpu.CompilerParams(vmem_limit_bytes=24 << 20),
        cost_estimate=pl.CostEstimate(flops=flops, bytes_accessed=10**5, transcendentals=0),
        name=name,
    )(*ins)


def body(tokens, gate_weights, expert_ids, gate_proj, up_proj, down_proj):
    groups, experts = lax.axis_size("dp"), lax.axis_size("ep")
    devices = groups * experts
    features, width = tokens.shape[3], gate_proj.shape[2]
    top, quarter = expert_ids.shape[3], features // 4
    bf16, f32 = jnp.bfloat16, jnp.float32
    gate, up, down = gate_proj[0], up_proj[0], down_proj[0]
    swap = [(i, i ^ 1) for i in range(experts)]
    heavy = 2 * 10**10

    small = call(
        read_kernel,
        "read",
        (
            jax.ShapeDtypeStruct((1, features), bf16),
            jax.ShapeDtypeStruct((1, top), bf16),
            jax.ShapeDtypeStruct((1, top), jnp.int32),
        ),
        tuple(
            pltpu.with_memory_space_constraint(x[0, 0], pltpu.HBM)
            for x in (tokens, gate_weights, expert_ids)
        ),
        10**4,
        [pltpu.SemaphoreType.DMA((3,))],
        [HBM] * 3,
    )
    sent = call(
        functools.partial(prepare_kernel, experts),
        "prepare",
        jax.ShapeDtypeStruct((devices, 2, quarter + LANES), bf16),
        small,
        heavy,
    )
    own = lax.all_to_all(sent, ("dp", "ep"), 0, 0, tiled=True)
    other = lax.ppermute(own, "ep", swap)
    acc = jax.ShapeDtypeStruct((2 * devices, width), f32)
    gate_acc, up_acc = call(first_kernel, "first", (acc, acc), (own, gate, up), heavy)
    hidden, out = call(
        second_kernel,
        "second",
        (
            jax.ShapeDtypeStruct((2 * devices, width), bf16),
            jax.ShapeDtypeStruct((devices, 2, quarter), bf16),
        ),
        (own, other, gate_acc, up_acc, gate, up, down),
        heavy,
    )
    received = lax.ppermute(out, "ep", swap)
    kept = call(
        third_kernel,
        "third",
        jax.ShapeDtypeStruct((2 * devices, quarter), f32),
        (hidden, own, down),
        heavy,
    )
    summed = call(
        add_kernel, "add", jax.ShapeDtypeStruct((devices, 2, quarter), bf16), (kept, received), 10**6
    )
    parts = lax.all_to_all(summed, ("dp", "ep"), 0, 0, tiled=True)
    mixed = call(mix_kernel, "mix", jax.ShapeDtypeStruct((1, features), bf16), (parts,), 10**6)
    return mixed[None, None]


def solution(mesh):
    placed = (
        P("ep", "dp", None, None),
        P("ep", "dp", None, None),
        P("ep", "dp", None, None),
        P("ep", None, "dp"),
        P("ep", None, "dp"),
        P("ep", "dp", None),
    )
    return jax.shard_map(
        body, mesh=mesh, in_specs=placed, out_specs=P("ep", "dp", None, None), check_vma=False
    )
```

```python
import functools
import math

import jax
import jax.numpy as jnp
from jax import lax
from jax.experimental import pallas as pl
from jax.experimental.pallas import tpu as pltpu
from jax.sharding import Mesh
from jax.sharding import PartitionSpec as P

LANES = 128
NEAR = 4
ORDER = ("near", "dp", "far")
VMEM = pl.BlockSpec(memory_space=pltpu.VMEM)
HBM = pl.BlockSpec(memory_space=pltpu.HBM)


def block(total, rows):
    return next(
        size
        for size in range(total, 0, -LANES)
        if total % size == 0 and (size == LANES or rows * size <= 1 << 17)
    )


def matmul(x, ref, start, columns):
    total = None
    for k in range(0, x.shape[1], LANES):
        part = jnp.dot(
            x[:, k : k + LANES],
            ref[pl.ds(pl.multiple_of(start + k, LANES), LANES), columns],
            preferred_element_type=jnp.float32,
        )
        total = part if total is None else total + part
    return total


def is_even(shape):
    return lax.rem(lax.broadcasted_iota(jnp.int32, shape, 0), 2) == 0


def parity():
    return lax.rem(lax.axis_index("near"), 2)


def part_of(index, size):
    return pl.ds(pl.multiple_of(index * size, size), size)


def read_kernel(*refs):
    sources, targets, sems = refs[:3], refs[3:6], refs[6]
    copies = [
        pltpu.make_async_copy(source, target, sems.at[i])
        for i, (source, target) in enumerate(zip(sources, targets))
    ]
    for copy in copies:
        copy.start()
    for copy in copies:
        copy.wait()


def prepare_kernel(far, tokens_ref, weights_ref, ids_ref, sent_ref):
    devices = sent_ref.shape[0]
    quarter = tokens_ref.shape[1] // 4
    row_index = lax.broadcasted_iota(jnp.int32, (2 * devices, ids_ref.shape[1]), 0)
    device = lax.div(row_index, 2)
    expert = lax.rem(device, far) * NEAR + lax.div(device, devices // NEAR)
    chosen = jnp.where(expert == ids_ref[...], weights_ref[...].astype(jnp.float32), 0.0)
    scale = jnp.broadcast_to(jnp.sum(chosen, axis=1, keepdims=True), (2 * devices, LANES))
    sent_ref[:, :, quarter:] = scale.astype(jnp.bfloat16).reshape(devices, 2, LANES)
    row = tokens_ref[...].astype(jnp.float32)
    quad = [row[:, i * quarter : (i + 1) * quarter] for i in range(4)]
    some = math.gcd(8, devices // NEAR)
    pairs = [
        jnp.concatenate(quad[2 * half : 2 * half + 2] * some, axis=0)
        .astype(jnp.bfloat16)
        .reshape(some, 2, quarter)
        for half in range(2)
    ]
    for i in range(0, devices, some):
        sent_ref[i : i + some, :, :quarter] = pairs[i // (devices // NEAR) % 2]


def project(rows, ref, half, columns):
    quarter = rows.shape[1]
    count = rows.shape[0]
    low = matmul(rows, ref, 2 * half * quarter, columns)
    high = matmul(rows, ref, (2 * half + 1) * quarter, columns)
    return jnp.where(
        is_even(low.shape), low + pltpu.roll(high, count - 1, 0), high + pltpu.roll(low, 1, 0)
    )


def half_rows(ref):
    devices, _, size = ref.shape
    return ref[:, :, : size - LANES].reshape(2 * devices, size - LANES)


def scale_of(ref):
    devices, _, size = ref.shape
    scale = ref[:, :, size - LANES :].reshape(2 * devices, LANES)
    return scale[:, :1].astype(jnp.float32)


def first_kernel(own_ref, gate_ref, up_ref, gate_acc_ref, up_acc_ref):
    rows, half = half_rows(own_ref), parity()
    width = gate_ref.shape[1]
    step = block(width, rows.shape[0])

    @pl.loop(0, width // step)
    def _(i):
        columns = part_of(i, step)
        gate_acc_ref[:, columns] = project(rows, gate_ref, half, columns)
        up_acc_ref[:, columns] = project(rows, up_ref, half, columns)


def project_down(hidden_ref, down_ref, scale, half, store):
    hidden = hidden_ref[...]
    quarter = down_ref.shape[1] // 4
    step = block(quarter, hidden.shape[0])

    if step == quarter:
        both = matmul(hidden, down_ref, 0, part_of(half, 2 * quarter))
        low, high = both[:, :quarter], both[:, quarter:]
        store(slice(None), jnp.where(is_even(low.shape), low, high) * scale)
        return

    @pl.loop(0, quarter // step)
    def _(i):
        start = pl.multiple_of(2 * half * quarter + i * step, LANES)
        low = matmul(hidden, down_ref, 0, pl.ds(start, step))
        high = matmul(hidden, down_ref, 0, pl.ds(start + quarter, step))
        store(part_of(i, step), jnp.where(is_even(low.shape), low, high) * scale)


def second_kernel(
    own_ref, other_ref, gate_acc_ref, up_acc_ref, gate_ref, up_ref, down_ref, hidden_ref, out_ref
):
    rows, half = half_rows(other_ref), 1 - parity()
    width = gate_ref.shape[1]
    step = block(width, rows.shape[0])

    @pl.loop(0, width // step)
    def _(i):
        columns = part_of(i, step)
        gate = gate_acc_ref[:, columns] + project(rows, gate_ref, half, columns)
        up = up_acc_ref[:, columns] + project(rows, up_ref, half, columns)
        hidden_ref[:, columns] = (gate / (1.0 + jnp.exp(-gate)) * up).astype(jnp.bfloat16)

    scale = scale_of(own_ref)

    def store(columns, value):
        devices = out_ref.shape[0]
        out_ref[:, :, columns] = value.astype(jnp.bfloat16).reshape(devices, 2, value.shape[1])

    project_down(hidden_ref, down_ref, scale, half, store)


def third_kernel(hidden_ref, scale_ref, down_ref, out_ref):
    def store(columns, value):
        out_ref[:, columns] = value

    project_down(hidden_ref, down_ref, scale_of(scale_ref), parity(), store)


def add_kernel(kept_ref, received_ref, out_ref):
    devices, _, quarter = received_ref.shape
    received = received_ref[...].reshape(2 * devices, quarter).astype(jnp.float32)
    out_ref[...] = (kept_ref[...] + received).astype(jnp.bfloat16).reshape(devices, 2, quarter)


def mix_kernel(parts_ref, out_ref):
    devices, _, quarter = parts_ref.shape
    rows = parts_ref[...].reshape(2 * devices, quarter).astype(jnp.float32)
    size = 2 * devices // NEAR
    for half in range(2):
        mine = sum(rows[i * size : (i + 1) * size] for i in range(half, NEAR, 2))
        mine = jnp.sum(mine.reshape(size // 8, 8, quarter), axis=0)
        mine = mine[:4] + mine[4:]
        mine = (mine[:2] + mine[2:]).astype(jnp.bfloat16)
        for i in range(2):
            start = (2 * half + i) * quarter
            out_ref[:, start : start + quarter] = mine[i : i + 1]


def call(kernel, name, outs, ins, flops, scratch=(), in_specs=None):
    return pl.pallas_call(
        kernel,
        out_shape=outs,
        in_specs=in_specs or [VMEM] * len(ins),
        out_specs=jax.tree.map(lambda _: VMEM, outs),
        scratch_shapes=scratch,
        compiler_params=pltpu.CompilerParams(vmem_limit_bytes=24 << 20),
        cost_estimate=pl.CostEstimate(flops=flops, bytes_accessed=10**5, transcendentals=0),
        name=name,
    )(*ins)


def body(tokens, gate_weights, expert_ids, gate_proj, up_proj, down_proj):
    far = lax.axis_size("far")
    devices = lax.axis_size("dp") * far * NEAR
    features, width = tokens.shape[3], gate_proj.shape[2]
    top, quarter = expert_ids.shape[3], features // 4
    bf16, f32 = jnp.bfloat16, jnp.float32
    gate, up, down = gate_proj[0], up_proj[0], down_proj[0]
    swap = [(i, i ^ 1) for i in range(NEAR)]
    heavy = 2 * 10**10

    small = call(
        read_kernel,
        "read",
        (
            jax.ShapeDtypeStruct((1, features), bf16),
            jax.ShapeDtypeStruct((1, top), bf16),
            jax.ShapeDtypeStruct((1, top), jnp.int32),
        ),
        tuple(
            pltpu.with_memory_space_constraint(x[0, 0], pltpu.HBM)
            for x in (tokens, gate_weights, expert_ids)
        ),
        10**4,
        [pltpu.SemaphoreType.DMA((3,))],
        [HBM] * 3,
    )
    sent = call(
        functools.partial(prepare_kernel, far),
        "prepare",
        jax.ShapeDtypeStruct((devices, 2, quarter + LANES), bf16),
        small,
        heavy,
    )
    own = lax.all_to_all(sent, ORDER, 0, 0, tiled=True)
    other = lax.ppermute(own, "near", swap)
    acc = jax.ShapeDtypeStruct((2 * devices, width), f32)
    gate_acc, up_acc = call(first_kernel, "first", (acc, acc), (own, gate, up), heavy)
    hidden, out = call(
        second_kernel,
        "second",
        (
            jax.ShapeDtypeStruct((2 * devices, width), bf16),
            jax.ShapeDtypeStruct((devices, 2, quarter), bf16),
        ),
        (own, other, gate_acc, up_acc, gate, up, down),
        heavy,
    )
    received = lax.ppermute(out, "near", swap)
    kept = call(
        third_kernel,
        "third",
        jax.ShapeDtypeStruct((2 * devices, quarter), f32),
        (hidden, own, down),
        heavy,
    )
    summed = call(
        add_kernel, "add", jax.ShapeDtypeStruct((devices, 2, quarter), bf16), (kept, received), 10**6
    )
    parts = lax.all_to_all(summed, ORDER, 0, 0, tiled=True)
    mixed = call(mix_kernel, "mix", jax.ShapeDtypeStruct((1, features), bf16), (parts,), 10**6)
    return mixed[None, None]


def solution(mesh):
    sizes = dict(mesh.shape)
    devices = mesh.devices.reshape(sizes["dp"], sizes["ep"] // NEAR, NEAR)
    split = Mesh(devices, ("dp", "far", "near"))
    experts = ("far", "near")
    placed = (
        P(experts, "dp", None, None),
        P(experts, "dp", None, None),
        P(experts, "dp", None, None),
        P(experts, None, "dp"),
        P(experts, None, "dp"),
        P(experts, "dp", None),
    )
    return jax.shard_map(
        body, mesh=split, in_specs=placed, out_specs=P(experts, "dp", None, None), check_vma=False
    )
```

```python
import functools
import math

import jax
import jax.numpy as jnp
from jax import lax
from jax.experimental import pallas as pl
from jax.experimental.pallas import tpu as pltpu
from jax.sharding import Mesh
from jax.sharding import PartitionSpec as P

LANES = 128
NEAR = 4
ORDER = ("near", "dp", "far")
VMEM = pl.BlockSpec(memory_space=pltpu.VMEM)
HBM = pl.BlockSpec(memory_space=pltpu.HBM)


def block(total, rows):
    return next(
        size
        for size in range(total, 0, -LANES)
        if total % size == 0 and (size == LANES or rows * size <= 1 << 17)
    )


def matmul(x, ref, start, columns):
    total = None
    for k in range(0, x.shape[1], LANES):
        part = jnp.dot(
            x[:, k : k + LANES],
            ref[pl.ds(pl.multiple_of(start + k, LANES), LANES), columns],
            preferred_element_type=jnp.float32,
        )
        total = part if total is None else total + part
    return total


def is_even(shape):
    return lax.rem(lax.broadcasted_iota(jnp.int32, shape, 0), 2) == 0


def parity():
    return lax.rem(lax.axis_index("near"), 2)


def part_of(index, size):
    return pl.ds(pl.multiple_of(index * size, size), size)


def read_kernel(*refs):
    sources, targets, sems = refs[:3], refs[3:6], refs[6]
    copies = [
        pltpu.make_async_copy(source, target, sems.at[i])
        for i, (source, target) in enumerate(zip(sources, targets))
    ]
    for copy in copies:
        copy.start()
    for copy in copies:
        copy.wait()


def prepare_kernel(far, tokens_ref, weights_ref, ids_ref, sent_ref):
    devices = sent_ref.shape[0]
    quarter = tokens_ref.shape[1] // 4
    row_index = lax.broadcasted_iota(jnp.int32, (2 * devices, ids_ref.shape[1]), 0)
    device = lax.div(row_index, 2)
    expert = lax.rem(device, far) * NEAR + lax.div(device, devices // NEAR)
    chosen = jnp.where(expert == ids_ref[...], weights_ref[...].astype(jnp.float32), 0.0)
    scale = jnp.broadcast_to(jnp.sum(chosen, axis=1, keepdims=True), (2 * devices, LANES))
    sent_ref[:, :, quarter:] = scale.astype(jnp.bfloat16).reshape(devices, 2, LANES)
    row = tokens_ref[...].astype(jnp.float32)
    quad = [row[:, i * quarter : (i + 1) * quarter] for i in range(4)]
    some = math.gcd(8, devices // NEAR)
    pairs = [
        jnp.concatenate(quad[2 * half : 2 * half + 2] * some, axis=0)
        .astype(jnp.bfloat16)
        .reshape(some, 2, quarter)
        for half in range(2)
    ]
    for i in range(0, devices, some):
        sent_ref[i : i + some, :, :quarter] = pairs[i // (devices // NEAR) % 2]


def project(rows, ref, half, columns):
    quarter = rows.shape[1]
    count = rows.shape[0]
    low = matmul(rows, ref, 2 * half * quarter, columns)
    high = matmul(rows, ref, (2 * half + 1) * quarter, columns)
    return jnp.where(
        is_even(low.shape), low + pltpu.roll(high, count - 1, 0), high + pltpu.roll(low, 1, 0)
    )


def half_rows(ref):
    devices, _, size = ref.shape
    return ref[:, :, : size - LANES].reshape(2 * devices, size - LANES)


def scale_of(ref):
    devices, _, size = ref.shape
    scale = ref[:, :, size - LANES :].reshape(2 * devices, LANES)
    return scale[:, :1].astype(jnp.float32)


def first_kernel(own_ref, gate_ref, up_ref, gate_acc_ref, up_acc_ref):
    rows, half = half_rows(own_ref), parity()
    width = gate_ref.shape[1]
    step = block(width, rows.shape[0])

    @pl.loop(0, width // step)
    def _(i):
        columns = part_of(i, step)
        gate_acc_ref[:, columns] = project(rows, gate_ref, half, columns)
        up_acc_ref[:, columns] = project(rows, up_ref, half, columns)


def project_down(hidden_ref, down_ref, scale, half, store):
    hidden = hidden_ref[...]
    quarter = down_ref.shape[1] // 4
    step = block(quarter, hidden.shape[0])

    if step == quarter:
        both = matmul(hidden, down_ref, 0, part_of(half, 2 * quarter))
        low, high = both[:, :quarter], both[:, quarter:]
        store(slice(None), jnp.where(is_even(low.shape), low, high) * scale)
        return

    @pl.loop(0, quarter // step)
    def _(i):
        start = pl.multiple_of(2 * half * quarter + i * step, LANES)
        low = matmul(hidden, down_ref, 0, pl.ds(start, step))
        high = matmul(hidden, down_ref, 0, pl.ds(start + quarter, step))
        store(part_of(i, step), jnp.where(is_even(low.shape), low, high) * scale)


def second_kernel(
    own_ref, other_ref, gate_acc_ref, up_acc_ref, gate_ref, up_ref, down_ref, hidden_ref, out_ref
):
    rows, half = half_rows(other_ref), 1 - parity()
    width = gate_ref.shape[1]
    step = min(512, block(width, rows.shape[0]))

    @pl.loop(0, width // step, unroll=True)
    def _(i):
        columns = part_of(i, step)
        gate = gate_acc_ref[:, columns] + project(rows, gate_ref, half, columns)
        up = up_acc_ref[:, columns] + project(rows, up_ref, half, columns)
        hidden_ref[:, columns] = (gate / (1.0 + jnp.exp(-gate)) * up).astype(jnp.bfloat16)

    scale = scale_of(own_ref)

    def store(columns, value):
        devices = out_ref.shape[0]
        out_ref[:, :, columns] = value.astype(jnp.bfloat16).reshape(devices, 2, value.shape[1])

    project_down(hidden_ref, down_ref, scale, half, store)


def third_kernel(hidden_ref, scale_ref, down_ref, out_ref):
    def store(columns, value):
        out_ref[:, columns] = value

    project_down(hidden_ref, down_ref, scale_of(scale_ref), parity(), store)


def add_kernel(kept_ref, received_ref, out_ref):
    devices, _, quarter = received_ref.shape
    received = received_ref[...].reshape(2 * devices, quarter).astype(jnp.float32)
    out_ref[...] = (kept_ref[...] + received).astype(jnp.bfloat16).reshape(devices, 2, quarter)


def mix_kernel(parts_ref, out_ref):
    devices, _, quarter = parts_ref.shape
    rows = parts_ref[...].reshape(2 * devices, quarter).astype(jnp.float32)
    size = 2 * devices // NEAR
    for half in range(2):
        mine = sum(rows[i * size : (i + 1) * size] for i in range(half, NEAR, 2))
        mine = jnp.sum(mine.reshape(size // 8, 8, quarter), axis=0)
        mine = mine[:4] + mine[4:]
        mine = (mine[:2] + mine[2:]).astype(jnp.bfloat16)
        for i in range(2):
            start = (2 * half + i) * quarter
            out_ref[:, start : start + quarter] = mine[i : i + 1]


def call(kernel, name, outs, ins, flops, scratch=(), in_specs=None):
    return pl.pallas_call(
        kernel,
        out_shape=outs,
        in_specs=in_specs or [VMEM] * len(ins),
        out_specs=jax.tree.map(lambda _: VMEM, outs),
        scratch_shapes=scratch,
        compiler_params=pltpu.CompilerParams(vmem_limit_bytes=24 << 20),
        cost_estimate=pl.CostEstimate(flops=flops, bytes_accessed=10**5, transcendentals=0),
        name=name,
    )(*ins)


def body(tokens, gate_weights, expert_ids, gate_proj, up_proj, down_proj):
    far = lax.axis_size("far")
    devices = lax.axis_size("dp") * far * NEAR
    features, width = tokens.shape[3], gate_proj.shape[2]
    top, quarter = expert_ids.shape[3], features // 4
    bf16, f32 = jnp.bfloat16, jnp.float32
    gate, up, down = gate_proj[0], up_proj[0], down_proj[0]
    swap = [(i, i ^ 1) for i in range(NEAR)]
    heavy = 2 * 10**10

    small = call(
        read_kernel,
        "read",
        (
            jax.ShapeDtypeStruct((1, features), bf16),
            jax.ShapeDtypeStruct((1, top), bf16),
            jax.ShapeDtypeStruct((1, top), jnp.int32),
        ),
        tuple(
            pltpu.with_memory_space_constraint(x[0, 0], pltpu.HBM)
            for x in (tokens, gate_weights, expert_ids)
        ),
        10**4,
        [pltpu.SemaphoreType.DMA((3,))],
        [HBM] * 3,
    )
    sent = call(
        functools.partial(prepare_kernel, far),
        "prepare",
        jax.ShapeDtypeStruct((devices, 2, quarter + LANES), bf16),
        small,
        heavy,
    )
    own = lax.all_to_all(sent, ORDER, 0, 0, tiled=True)
    other = lax.ppermute(own, "near", swap)
    acc = jax.ShapeDtypeStruct((2 * devices, width), f32)
    gate_acc, up_acc = call(first_kernel, "first", (acc, acc), (own, gate, up), heavy)
    hidden, out = call(
        second_kernel,
        "second",
        (
            jax.ShapeDtypeStruct((2 * devices, width), bf16),
            jax.ShapeDtypeStruct((devices, 2, quarter), bf16),
        ),
        (own, other, gate_acc, up_acc, gate, up, down),
        heavy,
    )
    received = lax.ppermute(out, "near", swap)
    kept = call(
        third_kernel,
        "third",
        jax.ShapeDtypeStruct((2 * devices, quarter), f32),
        (hidden, own, down),
        heavy,
    )
    summed = call(
        add_kernel, "add", jax.ShapeDtypeStruct((devices, 2, quarter), bf16), (kept, received), 10**6
    )
    parts = lax.all_to_all(summed, ORDER, 0, 0, tiled=True)
    mixed = call(mix_kernel, "mix", jax.ShapeDtypeStruct((1, features), bf16), (parts,), 10**6)
    return mixed[None, None]


def solution(mesh):
    sizes = dict(mesh.shape)
    devices = mesh.devices.reshape(sizes["dp"], sizes["ep"] // NEAR, NEAR)
    split = Mesh(devices, ("dp", "far", "near"))
    experts = ("far", "near")
    placed = (
        P(experts, "dp", None, None),
        P(experts, "dp", None, None),
        P(experts, "dp", None, None),
        P(experts, None, "dp"),
        P(experts, None, "dp"),
        P(experts, "dp", None),
    )
    return jax.shard_map(
        body, mesh=split, in_specs=placed, out_specs=P(experts, "dp", None, None), check_vma=False
    )
```
